512 devices in a mesh: groups: 2 (over y), seq: 16 (over z), vocab: 8 (over x), batch: 2 (over core).
Axes of the slice: x: 8, y: 2, z: 16, core: 2. Of those that a mesh axis runs over, the one named last changes fastest.
The devices are a block of a 8x8x16 slice.
Arguments:
- queries: bfloat16 [32, 3072, 3584], P(('groups', 'vocab', 'batch'), 'seq'), parts along dimension 0, may hold values from -300 to 300
- keys: bfloat16 [32, 3072, 512], P(('groups', 'vocab', 'batch'), 'seq'), parts along dimension 0, may hold values from -10 to 10
- values: bfloat16 [32, 3072, 512], P(('groups', 'vocab', 'batch'), 'seq'), parts along dimension 0, may hold values from -24 to 24
- residual: bfloat16 [32, 3072, 3584], P(('groups', 'vocab', 'batch'), 'seq'), parts along dimension 0, may hold values from -2048 to 2048
- norm_gain: float32 [3584], replicated, may hold values from 0.5 to 1.5
Outputs:
- normed: bfloat16 [32, 3072, 3584], P(('groups', 'vocab', 'batch'), 'seq'), parts along dimension 0
The draws below stay inside these ranges and needn't reach their ends.
There are 2 independent parts, one for each index of `groups`. The reference program is written for one: setup_inputs(seed, part) draws one part's arguments, and reference() takes and returns one part's arrays. A program takes and returns all parts, laid end to end along the dimension named above; an argument that names none is the same for every part. Nothing has to cross between parts.
All inputs are finite; a program needn't handle non-finite values.
Results may differ from the reference program's by a relative error of at most 0.0049.
Values may be sent and summed in bfloat16 or wider, within the bound.
No kernel may reach another device: no remote copies, remote signals or barrier semaphores. Data moves between devices by JAX's collectives and lax.ppermute only.
A program may use at most 128 MiB of HBM per device.

```python
import math
import jax
import jax.numpy as jnp
from jax import lax

D = 3584
QUERY_HEADS = 28
KEY_VALUE_HEADS = 4
HEAD_WIDTH = 128
RESPONSE_LENGTH = 3072
RESPONSE_COUNT = 16


def query_keys(key):
    key_start, key_query = jax.random.split(jax.random.fold_in(key, 11), 2)
    unscaled_keys = 1.5 * jax.random.truncated_normal(key_start, -6.0, 6.0, (RESPONSE_COUNT, RESPONSE_LENGTH, KEY_VALUE_HEADS, HEAD_WIDTH), jnp.float32)
    unscaled_query = 1.5 * jax.random.truncated_normal(key_query, -6.0, 6.0, (RESPONSE_COUNT, RESPONSE_LENGTH, QUERY_HEADS, HEAD_WIDTH), jnp.float32)
    return (unscaled_query.reshape(RESPONSE_COUNT, RESPONSE_LENGTH, QUERY_HEADS * HEAD_WIDTH), unscaled_keys.reshape(RESPONSE_COUNT, RESPONSE_LENGTH, KEY_VALUE_HEADS * HEAD_WIDTH))


def draw_queries(key, part):
    return query_keys(key)[0].astype(jnp.bfloat16)


def draw_keys(key, part):
    return query_keys(key)[1].astype(jnp.bfloat16)


def draw_residual(key, part):
    key_rows, key_columns, key_start = jax.random.split(jax.random.fold_in(key, 23), 3)
    row_scale = jnp.exp(jax.random.uniform(key_rows, (RESPONSE_COUNT, RESPONSE_LENGTH, 1), jnp.float32, math.log(0.3), math.log(3.0)))
    column_scale = jnp.exp(jax.random.uniform(key_columns, (1, 1, D), jnp.float32, math.log(0.3), math.log(3.0)))
    drawn = jax.random.truncated_normal(key_start, -6.0, 6.0, (RESPONSE_COUNT, RESPONSE_LENGTH, D), jnp.float32) * row_scale * column_scale
    return drawn.astype(jnp.bfloat16)


def block_levels(stream_key, dims, pieces, low, high):
    factor_of = 1.0
    for axis_at, parts in pieces:
        heights = jax.random.uniform(jax.random.fold_in(jax.random.fold_in(stream_key, 6), axis_at), (parts,), jnp.float32, low / len(pieces), high / len(pieces))
        factor_of = factor_of * jnp.repeat(jnp.exp(heights), dims[axis_at] // parts).reshape((-1,) + (1,) * (len(dims) - 1 - axis_at))
    return factor_of


def scatter_about(rng, shape, spread, bound, shards=(), held_as=jnp.bfloat16):
    gain = block_levels(rng, shape, shards, -0.22, 0.18) if shards else 1.0
    values = jax.random.normal(rng, shape, jnp.float32) * spread * gain
    return jnp.minimum(jnp.maximum(values, -bound), bound).astype(held_as)


def setup_inputs(seed: int = 0, part: int = 0) -> dict:
    splits = jax.random.split(jax.random.key(seed), 6)
    part_splits = jax.random.split(jax.random.fold_in(splits[5], part), 6)
    queries = draw_queries(jax.random.fold_in(jax.random.fold_in(splits[5], part), 71), part)
    keys = draw_keys(jax.random.fold_in(jax.random.fold_in(splits[5], part), 71), part)
    values = scatter_about(part_splits[2], (RESPONSE_COUNT, RESPONSE_LENGTH, KEY_VALUE_HEADS * HEAD_WIDTH), 4.0, 24.0, ((0, 16), (1, 16)))
    residual = draw_residual(jax.random.fold_in(jax.random.fold_in(splits[5], part), 71), part)
    norm_gain = jnp.clip(1.0 + 0.1 * jax.random.normal(splits[4], (D,), jnp.float32), 0.5, 1.5)
    return dict(queries=queries, keys=keys, values=values, residual=residual, norm_gain=norm_gain)


norm_eps = 1e-06

def reference(queries, keys, values, residual, norm_gain):
    queries_per_group = QUERY_HEADS // KEY_VALUE_HEADS
    position = jnp.arange(RESPONSE_LENGTH, dtype=jnp.int32)
    causal = position[None, :] <= position[:, None]

    def one_response(inputs):
        query_all, key_all, value_all = inputs

        def one_head(head_index):
            group_index = head_index // queries_per_group
            query_head = lax.dynamic_slice_in_dim(query_all, (head_index * HEAD_WIDTH).astype(jnp.int32), HEAD_WIDTH, 1)
            key_head = lax.dynamic_slice_in_dim(key_all, (group_index * HEAD_WIDTH).astype(jnp.int32), HEAD_WIDTH, 1)
            value_head = lax.dynamic_slice_in_dim(value_all, (group_index * HEAD_WIDTH).astype(jnp.int32), HEAD_WIDTH, 1)
            scores = jnp.dot(query_head, key_head.T, preferred_element_type=jnp.float32) * (1.0 / math.sqrt(HEAD_WIDTH))
            scores = jnp.where(causal, scores, -jnp.inf)
            row_max = lax.optimization_barrier(jnp.max(scores, axis=1, keepdims=True))
            weights = jnp.exp(scores - row_max)
            soft_probs = (weights / lax.optimization_barrier(jnp.sum(weights, axis=1, keepdims=True))).astype(jnp.bfloat16)
            return jnp.dot(soft_probs, value_head, preferred_element_type=jnp.float32).astype(jnp.bfloat16)
        heads_out = lax.map(one_head, jnp.arange(QUERY_HEADS, dtype=jnp.int32))
        return jnp.transpose(heads_out, (1, 0, 2)).reshape(RESPONSE_LENGTH, QUERY_HEADS * HEAD_WIDTH)
    attended = lax.map(one_response, (queries, keys, values))

    def one_norm(inputs):
        attended_rows, residual_rows = inputs
        hidden = residual_rows.astype(jnp.float32) + attended_rows.astype(jnp.float32)
        inv_rms = lax.rsqrt(lax.optimization_barrier(jnp.mean(hidden * hidden, axis=1, keepdims=True)) + norm_eps)
        return (hidden * inv_rms * norm_gain).astype(jnp.bfloat16)
    return lax.map(one_norm, (attended, residual))
```

```python
import functools
import math

import jax
import jax.numpy as jnp
from jax import lax
from jax.experimental import pallas as pl
from jax.experimental.pallas import tpu as pltpu
from jax.sharding import PartitionSpec as P


HEAD_WIDTH = 128
NORM_EPS = 1e-06
SCALE = math.log2(math.e) / math.sqrt(HEAD_WIDTH)
VMEM_LIMIT = 12 * 1024 * 1024


def lanes(col, width):
    reps = -(-width // HEAD_WIDTH)
    wide = jnp.concatenate([col] * reps, axis=1) if reps > 1 else col
    return wide[:, :width]


def attend(query, key, value_ones, old, causal):
    scores = lax.dot_general(query, key, (((1,), (1,)), ((), ())), preferred_element_type=jnp.float32)
    rows, width = scores.shape
    if causal:
        row = lax.broadcasted_iota(jnp.int32, scores.shape, 0)
        col = lax.broadcasted_iota(jnp.int32, scores.shape, 1)
        scores = jnp.where(col <= row, scores, -jnp.inf)
    top_here = jnp.max(scores, axis=1, keepdims=True) * SCALE
    if old is None:
        top = jnp.broadcast_to(top_here, (rows, HEAD_WIDTH))
    else:
        top = jnp.maximum(old[2], top_here)
    weights = jnp.exp2(scores * SCALE - lanes(top, width))
    summed = jnp.dot(weights.astype(jnp.bfloat16), value_ones, preferred_element_type=jnp.float32)
    acc, total = summed[:, :HEAD_WIDTH], summed[:, HEAD_WIDTH:]
    if old is not None:
        fade = jnp.exp2(old[2] - top)
        acc = old[0] * fade + acc
        total = old[1] * fade + total
    return acc, total, top


def group_key_value(blocks, group, kv_heads):
    key_at = pl.ds(pl.multiple_of(group * HEAD_WIDTH, HEAD_WIDTH), HEAD_WIDTH)
    value_at = pl.ds(pl.multiple_of((kv_heads + group) * HEAD_WIDTH, HEAD_WIDTH), HEAD_WIDTH)
    key = jnp.concatenate([b[:, key_at] for b in blocks], axis=0)
    value = jnp.concatenate([b[:, value_at] for b in blocks], axis=0)
    return key, jnp.concatenate([value, jnp.ones_like(value)], axis=1)


def each_head(q_ref, blocks, acc_ref, total_ref, top_ref, q_heads, kv_heads, first):
    per_group = q_heads // kv_heads

    def one_group(group, carry):
        key, value_ones = group_key_value(blocks, group, kv_heads)
        for i in range(per_group):
            head = group * per_group + i
            query = q_ref[:, pl.ds(pl.multiple_of(head * HEAD_WIDTH, HEAD_WIDTH), HEAD_WIDTH)]
            old = None if first else (acc_ref[head], total_ref[head], top_ref[head])
            acc, total, top = attend(query, key, value_ones, old, first)
            acc_ref[head] = acc
            total_ref[head] = total
            top_ref[head] = top
        return carry

    lax.fori_loop(0, kv_heads, one_group, 0)


def first_kernel(_place, q_ref, kv_ref, q_out, acc_ref, total_ref, top_ref, *, q_heads, kv_heads):
    q_out[...] = q_ref[...]
    each_head(q_ref, (kv_ref,), acc_ref, total_ref, top_ref, q_heads, kv_heads, True)


def step_kernel(place_ref, q_ref, f_ref, b_ref, _a, _t, _m, acc_ref, total_ref, top_ref, *, step, count, q_heads, kv_heads):
    place = place_ref[0]
    wrapped = place + step >= count

    @pl.when(wrapped)
    def _():
        each_head(q_ref, (f_ref, b_ref), acc_ref, total_ref, top_ref, q_heads, kv_heads, False)

    @pl.when(jnp.logical_and(place >= step, jnp.logical_not(wrapped)))
    def _():
        each_head(q_ref, (f_ref,), acc_ref, total_ref, top_ref, q_heads, kv_heads, False)


def last_kernel(
    place_ref, q_ref, f_ref, b_ref, residual_ref, gain_ref, _a, _t, _m, acc_ref, total_ref, top_ref, out_ref,
    *, step, q_heads, kv_heads,
):
    @pl.when(place_ref[0] >= step)
    def _():
        each_head(q_ref, (f_ref, b_ref), acc_ref, total_ref, top_ref, q_heads, kv_heads, False)

    rows, width = out_ref.shape
    square = jnp.zeros((rows, HEAD_WIDTH), jnp.float32)
    for head in range(q_heads):
        at = slice(head * HEAD_WIDTH, (head + 1) * HEAD_WIDTH)
        attended = (acc_ref[head] / total_ref[head]).astype(jnp.bfloat16).astype(jnp.float32)
        hidden = residual_ref[:, at].astype(jnp.float32) + attended
        acc_ref[head] = hidden
        square = square + hidden * hidden
    inv_rms = lax.rsqrt(jnp.sum(square, axis=1, keepdims=True) / width + NORM_EPS)
    inv_rms = jnp.broadcast_to(inv_rms, (rows, HEAD_WIDTH))
    for head in range(q_heads):
        at = slice(head * HEAD_WIDTH, (head + 1) * HEAD_WIDTH)
        out_ref[:, at] = (acc_ref[head] * inv_rms * gain_ref[:, at]).astype(jnp.bfloat16)


def shift(array, pairs):
    return lax.ppermute(array, "seq", pairs)


def layer(queries, keys, values, residual, norm_gain):
    count = lax.axis_size("seq")
    half = count // 2
    query = queries[0]
    rows, width = query.shape
    q_heads = width // HEAD_WIDTH
    kv_heads = keys.shape[2] // HEAD_WIDTH
    place = lax.axis_index("seq").astype(jnp.int32).reshape(1)
    own = jnp.concatenate([keys[0], values[0]], axis=1)
    right = [(i, (i + 1) % count) for i in range(count)]
    left = [(i, (i - 1) % count) for i in range(count)]
    state_shape = (q_heads, rows, HEAD_WIDTH)
    state = pltpu.VMEM(state_shape, jnp.float32)
    vmem = pl.BlockSpec(memory_space=pltpu.VMEM)
    smem = pl.BlockSpec(memory_space=pltpu.SMEM)
    params = pltpu.CompilerParams(vmem_limit_bytes=VMEM_LIMIT)

    def cost(keys_seen):
        return pl.CostEstimate(
            flops=4 * q_heads * rows * keys_seen * HEAD_WIDTH,
            transcendentals=q_heads * rows * keys_seen,
            bytes_accessed=4 * rows * width,
        )

    forward = shift(own, right)
    backward = shift(own, left)
    query, acc, total, top = pl.pallas_call(
        functools.partial(first_kernel, q_heads=q_heads, kv_heads=kv_heads),
        out_shape=(pltpu.VMEM(query.shape, query.dtype), state, state, state),
        in_specs=[smem, vmem, vmem],
        out_specs=(vmem, vmem, vmem, vmem),
        compiler_params=params,
        cost_estimate=cost(rows),
        name="first",
    )(place, query, own)
    for step in range(1, half):
        if step + 1 < half:
            forward_next = shift(forward, right)
            backward_next = shift(backward, left)
        else:
            forward_next = shift(forward[: rows // 2], right)
            backward_next = shift(backward[rows // 2 :], left)
        acc, total, top = pl.pallas_call(
            functools.partial(step_kernel, step=step, count=count, q_heads=q_heads, kv_heads=kv_heads),
            out_shape=(state, state, state),
            in_specs=[smem] + [vmem] * 6,
            out_specs=(vmem, vmem, vmem),
            input_output_aliases={4: 0, 5: 1, 6: 2},
            compiler_params=params,
            cost_estimate=cost(2 * rows),
        )(place, query, forward, backward, acc, total, top)
        forward, backward = forward_next, backward_next
    _, _, _, normed = pl.pallas_call(
        functools.partial(last_kernel, step=half, q_heads=q_heads, kv_heads=kv_heads),
        out_shape=(state, state, state, jax.ShapeDtypeStruct((rows, width), jnp.bfloat16)),
        in_specs=[smem] + [vmem] * 8,
        out_specs=(vmem, vmem, vmem, vmem),
        input_output_aliases={6: 0, 7: 1, 8: 2},
        compiler_params=params,
        cost_estimate=cost(rows),
        name="last",
    )(place, query, forward, backward, residual[0], norm_gain.reshape(1, width), acc, total, top)
    return normed[None]


def solution(mesh):
    placed = P(("groups", "vocab", "batch"), "seq", None)
    return jax.shard_map(
        layer,
        mesh=mesh,
        in_specs=(placed, placed, placed, placed, P()),
        out_specs=placed,
        check_vma=False,
    )
```

```python
import functools
import math

import jax
import jax.numpy as jnp
from jax import lax
from jax.experimental import pallas as pl
from jax.experimental.pallas import tpu as pltpu
from jax.sharding import PartitionSpec as P


HEAD_WIDTH = 128
NORM_EPS = 1e-06
SCALE = math.log2(math.e) / math.sqrt(HEAD_WIDTH)
VMEM_LIMIT = 12 * 1024 * 1024


def lanes(col, width):
    reps = -(-width // HEAD_WIDTH)
    wide = jnp.concatenate([col] * reps, axis=1) if reps > 1 else col
    return wide[:, :width]


def attend(query, key, value_ones, old, causal):
    scores = lax.dot_general(query, key, (((1,), (1,)), ((), ())), preferred_element_type=jnp.float32)
    rows, width = scores.shape
    if causal:
        row = lax.broadcasted_iota(jnp.int32, scores.shape, 0)
        col = lax.broadcasted_iota(jnp.int32, scores.shape, 1)
        scores = jnp.where(col <= row, scores, -jnp.inf)
    top_here = jnp.max(scores, axis=1, keepdims=True) * SCALE
    if old is None:
        top = jnp.broadcast_to(top_here, (rows, HEAD_WIDTH))
    else:
        top = jnp.maximum(old[2], top_here)
    weights = jnp.exp2(scores * SCALE - lanes(top, width))
    summed = jnp.dot(weights.astype(jnp.bfloat16), value_ones, preferred_element_type=jnp.float32)
    acc, total = summed[:, :HEAD_WIDTH], summed[:, HEAD_WIDTH:]
    if old is not None:
        fade = jnp.exp2(old[2] - top)
        acc = old[0] * fade + acc
        total = old[1] * fade + total
    return acc, total, top


def group_key_value(blocks, group, kv_heads):
    key_at = pl.ds(pl.multiple_of(group * HEAD_WIDTH, HEAD_WIDTH), HEAD_WIDTH)
    value_at = pl.ds(pl.multiple_of((kv_heads + group) * HEAD_WIDTH, HEAD_WIDTH), HEAD_WIDTH)
    key = jnp.concatenate([b[:, key_at] for b in blocks], axis=0)
    value = jnp.concatenate([b[:, value_at] for b in blocks], axis=0)
    return key, jnp.concatenate([value, jnp.ones_like(value)], axis=1)


def each_head(q_ref, blocks, acc_ref, total_ref, top_ref, q_heads, kv_heads, first):
    per_group = q_heads // kv_heads

    def one_group(group, carry):
        key, value_ones = group_key_value(blocks, group, kv_heads)
        for i in range(per_group):
            head = group * per_group + i
            query = q_ref[:, pl.ds(pl.multiple_of(head * HEAD_WIDTH, HEAD_WIDTH), HEAD_WIDTH)]
            old = None if first else (acc_ref[head], total_ref[head], top_ref[head])
            acc, total, top = attend(query, key, value_ones, old, first)
            acc_ref[head] = acc
            total_ref[head] = total
            top_ref[head] = top
        return carry

    lax.fori_loop(0, kv_heads, one_group, 0)


def first_kernel(_place, q_ref, kv_ref, q_out, acc_ref, total_ref, top_ref, *, q_heads, kv_heads):
    q_out[...] = q_ref[...]
    each_head(q_ref, (kv_ref,), acc_ref, total_ref, top_ref, q_heads, kv_heads, True)


def fold(place, step, count, f_ref, b_ref, update):
    behind = place >= step
    if b_ref is None:
        pl.when(behind)(lambda: update((f_ref,)))
    else:
        wrapped = place + step >= count
        pl.when(wrapped)(lambda: update((f_ref, b_ref)))
        pl.when(jnp.logical_and(behind, jnp.logical_not(wrapped)))(lambda: update((f_ref,)))


def step_kernel(place_ref, q_ref, f_ref, *refs, step, count, both, q_heads, kv_heads):
    b_ref = refs[0] if both else None
    state = refs[-3:]
    fold(
        place_ref[0], step, count, f_ref, b_ref,
        lambda blocks: each_head(q_ref, blocks, *state, q_heads, kv_heads, False),
    )


def last_kernel(place_ref, q_ref, f_ref, residual_ref, gain_ref, *refs, step, count, q_heads, kv_heads):
    acc_ref, total_ref, top_ref, out_ref = refs[-4:]
    fold(
        place_ref[0], step, count, f_ref, None,
        lambda blocks: each_head(q_ref, blocks, acc_ref, total_ref, top_ref, q_heads, kv_heads, False),
    )
    rows, width = out_ref.shape
    square = jnp.zeros((rows, HEAD_WIDTH), jnp.float32)
    for head in range(q_heads):
        at = slice(head * HEAD_WIDTH, (head + 1) * HEAD_WIDTH)
        attended = (acc_ref[head] / total_ref[head]).astype(jnp.bfloat16).astype(jnp.float32)
        hidden = residual_ref[:, at].astype(jnp.float32) + attended
        acc_ref[head] = hidden
        square = square + hidden * hidden
    inv_rms = lax.rsqrt(jnp.sum(square, axis=1, keepdims=True) / width + NORM_EPS)
    inv_rms = jnp.broadcast_to(inv_rms, (rows, HEAD_WIDTH))
    for head in range(q_heads):
        at = slice(head * HEAD_WIDTH, (head + 1) * HEAD_WIDTH)
        out_ref[:, at] = (acc_ref[head] * inv_rms * gain_ref[:, at]).astype(jnp.bfloat16)


def hops(count):
    backward = count * 3 // 8
    return count - 1 - backward, backward


def forward_pairs(count, step):
    return [(i, i + 1) for i in range(step - 1, count - 1)]


def backward_pairs(count, step, backward):
    return [(i, (i - 1) % count) for i in range(count) if (i + step - 1) % count < backward]


def shift(array, pairs):
    return lax.ppermute(array, "seq", pairs)


def layer(queries, keys, values, residual, norm_gain):
    count = lax.axis_size("seq")
    forward_steps, backward_steps = hops(count)
    query = queries[0]
    rows, width = query.shape
    q_heads = width // HEAD_WIDTH
    kv_heads = keys.shape[2] // HEAD_WIDTH
    place = lax.axis_index("seq").astype(jnp.int32).reshape(1)
    own = jnp.concatenate([keys[0], values[0]], axis=1)
    state_shape = (q_heads, rows, HEAD_WIDTH)
    state = pltpu.VMEM(state_shape, jnp.float32)
    vmem = pl.BlockSpec(memory_space=pltpu.VMEM)
    smem = pl.BlockSpec(memory_space=pltpu.SMEM)
    params = pltpu.CompilerParams(vmem_limit_bytes=VMEM_LIMIT)

    def cost(keys_seen):
        return pl.CostEstimate(
            flops=4 * q_heads * rows * keys_seen * HEAD_WIDTH,
            transcendentals=q_heads * rows * keys_seen,
            bytes_accessed=4 * rows * width,
        )

    forward = shift(own, forward_pairs(count, 1))
    backward = shift(own, backward_pairs(count, 1, backward_steps))
    query, acc, total, top = pl.pallas_call(
        functools.partial(first_kernel, q_heads=q_heads, kv_heads=kv_heads),
        out_shape=(pltpu.VMEM(query.shape, query.dtype), state, state, state),
        in_specs=[smem, vmem, vmem],
        out_specs=(vmem, vmem, vmem, vmem),
        compiler_params=params,
        cost_estimate=cost(rows),
        name="first",
    )(place, query, own)
    for step in range(1, forward_steps):
        blocks = (forward, backward) if step <= backward_steps else (forward,)
        forward = shift(forward, forward_pairs(count, step + 1))
        if step < backward_steps:
            backward = shift(backward, backward_pairs(count, step + 1, backward_steps))
        at = 2 + len(blocks)
        acc, total, top = pl.pallas_call(
            functools.partial(
                step_kernel, step=step, count=count, both=len(blocks) == 2, q_heads=q_heads, kv_heads=kv_heads
            ),
            out_shape=(state, state, state),
            in_specs=[smem] + [vmem] * (at + 2),
            out_specs=(vmem, vmem, vmem),
            input_output_aliases={at: 0, at + 1: 1, at + 2: 2},
            compiler_params=params,
            cost_estimate=cost(len(blocks) * rows),
        )(place, query, *blocks, acc, total, top)
    _, _, _, normed = pl.pallas_call(
        functools.partial(last_kernel, step=forward_steps, count=count, q_heads=q_heads, kv_heads=kv_heads),
        out_shape=(state, state, state, jax.ShapeDtypeStruct((rows, width), jnp.bfloat16)),
        in_specs=[smem] + [vmem] * 7,
        out_specs=(vmem, vmem, vmem, vmem),
        input_output_aliases={5: 0, 6: 1, 7: 2},
        compiler_params=params,
        cost_estimate=cost(rows),
        name="last",
    )(place, query, forward, residual[0], norm_gain.reshape(1, width), acc, total, top)
    return normed[None]


def solution(mesh):
    placed = P(("groups", "vocab", "batch"), "seq", None)
    return jax.shard_map(
        layer,
        mesh=mesh,
        in_specs=(placed, placed, placed, placed, P()),
        out_specs=placed,
        check_vma=False,
    )
```

```python
import functools
import math

import jax
import jax.numpy as jnp
from jax import lax
from jax.experimental import pallas as pl
from jax.experimental.pallas import tpu as pltpu
from jax.sharding import PartitionSpec as P


HEAD_WIDTH = 128
NORM_EPS = 1e-06
SCALE = math.log2(math.e) / math.sqrt(HEAD_WIDTH)
VMEM_LIMIT = 12 * 1024 * 1024


def lanes(col, width):
    reps = -(-width // HEAD_WIDTH)
    wide = jnp.concatenate([col] * reps, axis=1) if reps > 1 else col
    return wide[:, :width]


def lane_sums(weights):
    width = weights.shape[1]
    whole = width - width % HEAD_WIDTH
    part = weights[:, :HEAD_WIDTH]
    for at in range(HEAD_WIDTH, whole, HEAD_WIDTH):
        part = part + weights[:, at : at + HEAD_WIDTH]
    if whole < width:
        rest = weights[:, whole:]
        fill = jnp.zeros((rest.shape[0], HEAD_WIDTH - rest.shape[1]), jnp.float32)
        part = part + jnp.concatenate([rest, fill], axis=1)
    return part


def each_head(q_ref, keys, values, acc_ref, total_ref, top_ref, q_heads, kv_heads, first):
    per_group = q_heads // kv_heads

    def column(ref, start, group):
        return ref[:, pl.ds(pl.multiple_of(start + group * HEAD_WIDTH, HEAD_WIDTH), HEAD_WIDTH)]

    def one_group(group, carry):
        key = jnp.concatenate([column(ref, start, group) for ref, start in keys], axis=0)
        value = jnp.concatenate([column(ref, start, group) for ref, start in values], axis=0)

        def score(i):
            query = column(q_ref, 0, group * per_group + i)
            scores = lax.dot_general(query, key, (((1,), (1,)), ((), ())), preferred_element_type=jnp.float32)
            if first:
                row = lax.broadcasted_iota(jnp.int32, scores.shape, 0)
                col = lax.broadcasted_iota(jnp.int32, scores.shape, 1)
                scores = jnp.where(col <= row, scores, -jnp.inf)
            return scores

        def weigh(i, scores):
            head = group * per_group + i
            rows, width = scores.shape
            top_here = jnp.max(scores, axis=1, keepdims=True) * SCALE
            if first:
                top, fade = jnp.broadcast_to(top_here, (rows, HEAD_WIDTH)), None
            else:
                top = jnp.maximum(top_ref[head], top_here)
                fade = jnp.exp2(top_ref[head] - top)
            top_ref[head] = top
            return jnp.exp2(scores * SCALE - lanes(top, width)), fade

        def add(i, weights, fade):
            head = group * per_group + i
            acc = jnp.dot(weights.astype(jnp.bfloat16), value, preferred_element_type=jnp.float32)
            total = lane_sums(weights)
            acc_ref[head] = acc if first else acc_ref[head] * fade + acc
            total_ref[head] = total if first else total_ref[head] * fade + total

        scores = [score(0), score(1)]
        waiting = None
        for i in range(per_group):
            if i + 2 < per_group:
                scores.append(score(i + 2))
            weighed = weigh(i, scores[i])
            scores[i] = None
            if waiting is not None:
                add(*waiting)
            waiting = (i, *weighed)
        add(*waiting)
        return carry

    lax.fori_loop(0, kv_heads, one_group, 0)


def first_kernel(_place, q_ref, k_ref, v_ref, q_out, acc_ref, total_ref, top_ref, *, q_heads, kv_heads):
    q_out[...] = q_ref[...]
    each_head(q_ref, ((k_ref, 0),), ((v_ref, 0),), acc_ref, total_ref, top_ref, q_heads, kv_heads, True)


def fold(place, step, count, k_ref, v_ref, b_ref, update):
    behind = place >= step
    keys, values = ((k_ref, 0),), ((v_ref, 0),)
    if b_ref is None:
        pl.when(behind)(lambda: update(keys, values))
    else:
        wrapped = place + step >= count
        wide = b_ref.shape[1] // 2
        pl.when(wrapped)(lambda: update(keys + ((b_ref, 0),), values + ((b_ref, wide),)))
        pl.when(jnp.logical_and(behind, jnp.logical_not(wrapped)))(lambda: update(keys, values))


def step_kernel(place_ref, q_ref, k_ref, v_ref, *refs, step, count, both, q_heads, kv_heads):
    b_ref = refs[0] if both else None
    state = refs[-3:]
    fold(
        place_ref[0], step, count, k_ref, v_ref, b_ref,
        lambda keys, values: each_head(q_ref, keys, values, *state, q_heads, kv_heads, False),
    )


def last_kernel(place_ref, q_ref, k_ref, v_ref, residual_ref, gain_ref, *refs, step, count, q_heads, kv_heads):
    acc_ref, total_ref, top_ref, out_ref = refs[-4:]
    fold(
        place_ref[0], step, count, k_ref, v_ref, None,
        lambda keys, values: each_head(
            q_ref, keys, values, acc_ref, total_ref, top_ref, q_heads, kv_heads, False
        ),
    )
    rows, width = out_ref.shape
    square = jnp.zeros((rows, HEAD_WIDTH), jnp.float32)
    for head in range(q_heads):
        at = slice(head * HEAD_WIDTH, (head + 1) * HEAD_WIDTH)
        total = jnp.sum(total_ref[head], axis=1, keepdims=True)
        attended = (acc_ref[head] / total).astype(jnp.bfloat16).astype(jnp.float32)
        hidden = residual_ref[:, at].astype(jnp.float32) + attended
        acc_ref[head] = hidden
        square = square + hidden * hidden
    inv_rms = lax.rsqrt(jnp.sum(square, axis=1, keepdims=True) / width + NORM_EPS)
    inv_rms = jnp.broadcast_to(inv_rms, (rows, HEAD_WIDTH))
    for head in range(q_heads):
        at = slice(head * HEAD_WIDTH, (head + 1) * HEAD_WIDTH)
        out_ref[:, at] = (acc_ref[head] * inv_rms * gain_ref[:, at]).astype(jnp.bfloat16)


def hops(count):
    backward = count * 3 // 8
    return count - 1 - backward, backward


def forward_pairs(count, step):
    return [(i, i + 1) for i in range(step - 1, count - 1)]


def backward_pairs(count, step, backward):
    return [(i, (i - 1) % count) for i in range(count) if (i + step - 1) % count < backward]


def shift(array, pairs):
    return lax.ppermute(array, "seq", pairs)


def layer(queries, keys, values, residual, norm_gain):
    count = lax.axis_size("seq")
    forward_steps, backward_steps = hops(count)
    query = queries[0]
    rows, width = query.shape
    q_heads = width // HEAD_WIDTH
    kv_heads = keys.shape[2] // HEAD_WIDTH
    place = lax.axis_index("seq").astype(jnp.int32).reshape(1)
    key, value = keys[0], values[0]
    own = jnp.concatenate([key, value], axis=1)
    state_shape = (q_heads, rows, HEAD_WIDTH)
    state = pltpu.VMEM(state_shape, jnp.float32)
    vmem = pl.BlockSpec(memory_space=pltpu.VMEM)
    smem = pl.BlockSpec(memory_space=pltpu.SMEM)
    params = pltpu.CompilerParams(vmem_limit_bytes=VMEM_LIMIT)

    def cost(keys_seen):
        return pl.CostEstimate(
            flops=4 * q_heads * rows * keys_seen * HEAD_WIDTH,
            transcendentals=q_heads * rows * keys_seen,
            bytes_accessed=4 * rows * width,
        )

    key_here = shift(key, forward_pairs(count, 1))
    value_here = shift(value, forward_pairs(count, 1))
    backward = shift(own, backward_pairs(count, 1, backward_steps))
    query, acc, total, top = pl.pallas_call(
        functools.partial(first_kernel, q_heads=q_heads, kv_heads=kv_heads),
        out_shape=(pltpu.VMEM(query.shape, query.dtype), state, state, state),
        in_specs=[smem, vmem, vmem, vmem],
        out_specs=(vmem, vmem, vmem, vmem),
        compiler_params=params,
        cost_estimate=cost(rows),
        name="first",
    )(place, query, key, value)
    for step in range(1, forward_steps):
        blocks = (key_here, value_here, backward) if step <= backward_steps else (key_here, value_here)
        key_here = shift(key_here, forward_pairs(count, step + 1))
        value_here = shift(value_here, forward_pairs(count, step + 1))
        if step < backward_steps:
            backward = shift(backward, backward_pairs(count, step + 1, backward_steps))
        at = 2 + len(blocks)
        acc, total, top = pl.pallas_call(
            functools.partial(
                step_kernel, step=step, count=count, both=len(blocks) == 3, q_heads=q_heads, kv_heads=kv_heads
            ),
            out_shape=(state, state, state),
            in_specs=[smem] + [vmem] * (at + 2),
            out_specs=(vmem, vmem, vmem),
            input_output_aliases={at: 0, at + 1: 1, at + 2: 2},
            compiler_params=params,
            cost_estimate=cost((len(blocks) - 1) * rows),
        )(place, query, *blocks, acc, total, top)
    _, _, _, normed = pl.pallas_call(
        functools.partial(last_kernel, step=forward_steps, count=count, q_heads=q_heads, kv_heads=kv_heads),
        out_shape=(state, state, state, jax.ShapeDtypeStruct((rows, width), jnp.bfloat16)),
        in_specs=[smem] + [vmem] * 8,
        out_specs=(vmem, vmem, vmem, vmem),
        input_output_aliases={6: 0, 7: 1, 8: 2},
        compiler_params=params,
        cost_estimate=cost(rows),
        name="last",
    )(place, query, key_here, value_here, residual[0], norm_gain.reshape(1, width), acc, total, top)
    return normed[None]


def solution(mesh):
    placed = P(("groups", "vocab", "batch"), "seq", None)
    return jax.shard_map(
        layer,
        mesh=mesh,
        in_specs=(placed, placed, placed, placed, P()),
        out_specs=placed,
        check_vma=False,
    )
```

```python
import functools
import math

import jax
import jax.numpy as jnp
from jax import lax
from jax.experimental import pallas as pl
from jax.experimental.pallas import tpu as pltpu
from jax.sharding import PartitionSpec as P


HEAD_WIDTH = 128
NORM_EPS = 1e-06
SCALE = math.log2(math.e) / math.sqrt(HEAD_WIDTH)
VMEM_LIMIT = 12 * 1024 * 1024


def lanes(col, width):
    reps = -(-width // HEAD_WIDTH)
    wide = jnp.concatenate([col] * reps, axis=1) if reps > 1 else col
    return wide[:, :width]


def lane_sums(weights):
    width = weights.shape[1]
    whole = width - width % HEAD_WIDTH
    part = weights[:, :HEAD_WIDTH]
    for at in range(HEAD_WIDTH, whole, HEAD_WIDTH):
        part = part + weights[:, at : at + HEAD_WIDTH]
    if whole < width:
        rest = weights[:, whole:]
        fill = jnp.zeros((rest.shape[0], HEAD_WIDTH - rest.shape[1]), jnp.float32)
        part = part + jnp.concatenate([rest, fill], axis=1)
    return part


def each_head(q_ref, keys, values, acc_ref, total_ref, top_ref, q_heads, kv_heads, first):
    per_group = q_heads // kv_heads

    def column(ref, start, group):
        return ref[:, pl.ds(pl.multiple_of(start + group * HEAD_WIDTH, HEAD_WIDTH), HEAD_WIDTH)]

    def one_group(group, carry):
        key = jnp.concatenate([column(ref, start, group) for ref, start in keys], axis=0)
        value = jnp.concatenate([column(ref, start, group) for ref, start in values], axis=0)

        def score(i):
            query = column(q_ref, 0, group * per_group + i)
            scores = lax.dot_general(query, key, (((1,), (1,)), ((), ())), preferred_element_type=jnp.float32)
            if first:
                row = lax.broadcasted_iota(jnp.int32, scores.shape, 0)
                col = lax.broadcasted_iota(jnp.int32, scores.shape, 1)
                scores = jnp.where(col <= row, scores, -jnp.inf)
            return scores

        def weigh(i, scores):
            head = group * per_group + i
            rows, width = scores.shape
            top_here = jnp.max(scores, axis=1, keepdims=True) * SCALE
            if first:
                top, fade = jnp.broadcast_to(top_here, (rows, HEAD_WIDTH)), None
            else:
                top = jnp.maximum(top_ref[head], top_here)
                fade = jnp.exp2(top_ref[head] - top)
            top_ref[head] = top
            return jnp.exp2(scores * SCALE - lanes(top, width)), fade

        def add(i, weights, fade):
            head = group * per_group + i
            acc = jnp.dot(weights.astype(jnp.bfloat16), value, preferred_element_type=jnp.float32)
            total = lane_sums(weights)
            acc_ref[head] = acc if first else acc_ref[head] * fade + acc
            total_ref[head] = total if first else total_ref[head] * fade + total

        scores = [score(0), score(1)]
        waiting = None
        for i in range(per_group):
            if i + 2 < per_group:
                scores.append(score(i + 2))
            weighed = weigh(i, scores[i])
            scores[i] = None
            if waiting is not None:
                add(*waiting)
            waiting = (i, *weighed)
        add(*waiting)
        return carry

    lax.fori_loop(0, kv_heads, one_group, 0)


def first_kernel(_place, q_ref, own_ref, q_out, acc_ref, total_ref, top_ref, *, q_heads, kv_heads):
    q_out[...] = q_ref[...]
    wide = own_ref.shape[1] // 2
    each_head(q_ref, ((own_ref, 0),), ((own_ref, wide),), acc_ref, total_ref, top_ref, q_heads, kv_heads, True)


def fold(place, step, turn, count, f_ref, b_ref, update):
    behind = place >= step
    wide = f_ref.shape[1] // 2
    keys, values = ((f_ref, 0),), ((f_ref, wide),)
    if b_ref is None:
        pl.when(behind)(lambda: update(keys, values))
    else:
        wrapped = place + turn >= count
        pl.when(wrapped)(lambda: update(keys + ((b_ref, 0),), values + ((b_ref, wide),)))
        pl.when(jnp.logical_and(behind, jnp.logical_not(wrapped)))(lambda: update(keys, values))


def merge_kernel(place_ref, direct_ref, passed_ref, out_ref, *, count):
    last = place_ref[0] == count - 1

    @pl.when(last)
    def _():
        out_ref[...] = direct_ref[...]

    @pl.when(jnp.logical_not(last))
    def _():
        out_ref[...] = passed_ref[...]


def step_kernel(place_ref, q_ref, f_ref, *refs, step, turn, count, q_heads, kv_heads):
    b_ref = refs[0] if turn else None
    state = refs[-3:]
    fold(
        place_ref[0], step, turn, count, f_ref, b_ref,
        lambda keys, values: each_head(q_ref, keys, values, *state, q_heads, kv_heads, False),
    )


def last_kernel(place_ref, q_ref, f_ref, residual_ref, gain_ref, *refs, step, count, q_heads, kv_heads):
    acc_ref, total_ref, top_ref, out_ref = refs[-4:]
    fold(
        place_ref[0], step, None, count, f_ref, None,
        lambda keys, values: each_head(
            q_ref, keys, values, acc_ref, total_ref, top_ref, q_heads, kv_heads, False
        ),
    )
    rows, width = out_ref.shape
    square = jnp.zeros((rows, HEAD_WIDTH), jnp.float32)
    for head in range(q_heads):
        at = slice(head * HEAD_WIDTH, (head + 1) * HEAD_WIDTH)
        total = jnp.sum(total_ref[head], axis=1, keepdims=True)
        attended = (acc_ref[head] / total).astype(jnp.bfloat16).astype(jnp.float32)
        hidden = residual_ref[:, at].astype(jnp.float32) + attended
        acc_ref[head] = hidden
        square = square + hidden * hidden
    inv_rms = lax.rsqrt(jnp.sum(square, axis=1, keepdims=True) / width + NORM_EPS)
    inv_rms = jnp.broadcast_to(inv_rms, (rows, HEAD_WIDTH))
    for head in range(q_heads):
        at = slice(head * HEAD_WIDTH, (head + 1) * HEAD_WIDTH)
        out_ref[:, at] = (acc_ref[head] * inv_rms * gain_ref[:, at]).astype(jnp.bfloat16)


def plan(count):
    wrapped = count * 6 // 16
    forward = count - 1 - wrapped
    folds = [min(2 * turn, forward - 1 - (wrapped - turn)) for turn in range(1, wrapped + 1)]
    return forward, wrapped, folds


def forward_pairs(count, step):
    return [(i, i + 1) for i in range(step - 1, count - 1)]


def pass_pairs(count, turn):
    return [(count - 1 - i, count - 2 - i) for i in range(turn)]


def shift(array, pairs):
    return lax.ppermute(array, "seq", pairs)


def layer(queries, keys, values, residual, norm_gain):
    count = lax.axis_size("seq")
    forward_steps, wrapped_blocks, folds = plan(count)
    query = queries[0]
    rows, width = query.shape
    q_heads = width // HEAD_WIDTH
    kv_heads = keys.shape[2] // HEAD_WIDTH
    place = lax.axis_index("seq").astype(jnp.int32).reshape(1)
    own = jnp.concatenate([keys[0], values[0]], axis=1)
    state_shape = (q_heads, rows, HEAD_WIDTH)
    state = pltpu.VMEM(state_shape, jnp.float32)
    vmem = pl.BlockSpec(memory_space=pltpu.VMEM)
    smem = pl.BlockSpec(memory_space=pltpu.SMEM)
    params = pltpu.CompilerParams(vmem_limit_bytes=VMEM_LIMIT)

    def cost(keys_seen):
        return pl.CostEstimate(
            flops=4 * q_heads * rows * keys_seen * HEAD_WIDTH,
            transcendentals=q_heads * rows * keys_seen,
            bytes_accessed=4 * rows * width,
        )

    forward = shift(own, forward_pairs(count, 1))
    direct = [shift(own, [(0, count - 1)])]
    query, acc, total, top = pl.pallas_call(
        functools.partial(first_kernel, q_heads=q_heads, kv_heads=kv_heads),
        out_shape=(pltpu.VMEM(query.shape, query.dtype), state, state, state),
        in_specs=[smem, vmem, vmem],
        out_specs=(vmem, vmem, vmem, vmem),
        compiler_params=params,
        cost_estimate=cost(rows),
        name="first",
    )(place, query, own)
    passed = None
    for step in range(1, forward_steps):
        blocks = (forward,)
        forward = shift(forward, forward_pairs(count, step + 1))
        if step < wrapped_blocks:
            direct.append(shift(own, [(step, count - 1)]))
        turn = folds.index(step) + 1 if step in folds else None
        if turn:
            merged = direct[turn - 1]
            if passed is not None:
                merged = pl.pallas_call(
                    functools.partial(merge_kernel, count=count),
                    out_shape=pltpu.VMEM(own.shape, own.dtype),
                    in_specs=[smem, vmem, vmem],
                    out_specs=vmem,
                    compiler_params=params,
                    cost_estimate=pl.CostEstimate(flops=own.size, transcendentals=0, bytes_accessed=4 * own.size),
                )(place, merged, passed)
            if turn < wrapped_blocks:
                passed = shift(merged, pass_pairs(count, turn))
            blocks = blocks + (merged,)
        at = 2 + len(blocks)
        acc, total, top = pl.pallas_call(
            functools.partial(
                step_kernel, step=step, turn=turn, count=count, q_heads=q_heads, kv_heads=kv_heads
            ),
            out_shape=(state, state, state),
            in_specs=[smem] + [vmem] * (at + 2),
            out_specs=(vmem, vmem, vmem),
            input_output_aliases={at: 0, at + 1: 1, at + 2: 2},
            compiler_params=params,
            cost_estimate=cost(len(blocks) * rows),
        )(place, query, *blocks, acc, total, top)
    _, _, _, normed = pl.pallas_call(
        functools.partial(last_kernel, step=forward_steps, count=count, q_heads=q_heads, kv_heads=kv_heads),
        out_shape=(state, state, state, jax.ShapeDtypeStruct((rows, width), jnp.bfloat16)),
        in_specs=[smem] + [vmem] * 7,
        out_specs=(vmem, vmem, vmem, vmem),
        input_output_aliases={5: 0, 6: 1, 7: 2},
        compiler_params=params,
        cost_estimate=cost(rows),
        name="last",
    )(place, query, forward, residual[0], norm_gain.reshape(1, width), acc, total, top)
    return normed[None]


def solution(mesh):
    placed = P(("groups", "vocab", "batch"), "seq", None)
    return jax.shard_map(
        layer,
        mesh=mesh,
        in_specs=(placed, placed, placed, placed, P()),
        out_specs=placed,
        check_vma=False,
    )
```

```python
import functools
import math

import jax
import jax.numpy as jnp
from jax import lax
from jax.experimental import pallas as pl
from jax.experimental.pallas import tpu as pltpu
from jax.sharding import PartitionSpec as P


HEAD_WIDTH = 128
NORM_EPS = 1e-06
SCALE = math.log2(math.e) / math.sqrt(HEAD_WIDTH)
VMEM_LIMIT = 12 * 1024 * 1024


def lanes(col, width):
    reps = -(-width // HEAD_WIDTH)
    wide = jnp.concatenate([col] * reps, axis=1) if reps > 1 else col
    return wide[:, :width]


def lane_sums(weights):
    width = weights.shape[1]
    whole = width - width % HEAD_WIDTH
    part = weights[:, :HEAD_WIDTH]
    for at in range(HEAD_WIDTH, whole, HEAD_WIDTH):
        part = part + weights[:, at : at + HEAD_WIDTH]
    if whole < width:
        rest = weights[:, whole:]
        fill = jnp.zeros((rest.shape[0], HEAD_WIDTH - rest.shape[1]), jnp.float32)
        part = part + jnp.concatenate([rest, fill], axis=1)
    return part


def each_head(q_ref, keys, values, acc_ref, total_ref, top_ref, q_heads, kv_heads, first, finish=None):
    per_group = q_heads // kv_heads

    def column(ref, start, group):
        return ref[:, pl.ds(pl.multiple_of(start + group * HEAD_WIDTH, HEAD_WIDTH), HEAD_WIDTH)]

    def one_group(group, carry):
        key = jnp.concatenate([column(ref, start, group) for ref, start in keys], axis=0)
        value = jnp.concatenate([column(ref, start, group) for ref, start in values], axis=0)

        def score(i):
            query = column(q_ref, 0, group * per_group + i)
            scores = lax.dot_general(query, key, (((1,), (1,)), ((), ())), preferred_element_type=jnp.float32)
            if first:
                row = lax.broadcasted_iota(jnp.int32, scores.shape, 0)
                col = lax.broadcasted_iota(jnp.int32, scores.shape, 1)
                scores = jnp.where(col <= row, scores, -jnp.inf)
            return scores

        def weigh(i, scores):
            head = group * per_group + i
            rows, width = scores.shape
            top_here = jnp.max(scores, axis=1, keepdims=True) * SCALE
            if first:
                top, fade = jnp.broadcast_to(top_here, (rows, HEAD_WIDTH)), None
            else:
                top = jnp.maximum(top_ref[head], top_here)
                fade = jnp.exp2(top_ref[head] - top)
            if finish is None:
                top_ref[head] = top
            return jnp.exp2(scores * SCALE - lanes(top, width)), fade

        def add(i, weights, fade):
            head = group * per_group + i
            acc = jnp.dot(weights.astype(jnp.bfloat16), value, preferred_element_type=jnp.float32)
            total = lane_sums(weights)
            if not first:
                acc = acc_ref[head] * fade + acc
                total = total_ref[head] * fade + total
            if finish is None:
                acc_ref[head] = acc
                total_ref[head] = total
            else:
                finish(head, acc, total)

        scores = [score(0), score(1)]
        waiting = None
        for i in range(per_group):
            if i + 2 < per_group:
                scores.append(score(i + 2))
            weighed = weigh(i, scores[i])
            scores[i] = None
            if waiting is not None:
                add(*waiting)
            waiting = (i, *weighed)
        add(*waiting)
        return carry

    lax.fori_loop(0, kv_heads, one_group, 0)


def first_kernel(_place, q_ref, own_ref, q_out, acc_ref, total_ref, top_ref, *, q_heads, kv_heads):
    q_out[...] = q_ref[...]
    wide = own_ref.shape[1] // 2
    each_head(q_ref, ((own_ref, 0),), ((own_ref, wide),), acc_ref, total_ref, top_ref, q_heads, kv_heads, True)


def fold(place, step, turn, count, f_ref, b_ref, update):
    behind = place >= step
    wide = f_ref.shape[1] // 2
    keys, values = ((f_ref, 0),), ((f_ref, wide),)
    if b_ref is None:
        pl.when(behind)(lambda: update(keys, values))
    else:
        wrapped = place + turn >= count
        pl.when(wrapped)(lambda: update(keys + ((b_ref, 0),), values + ((b_ref, wide),)))
        pl.when(jnp.logical_and(behind, jnp.logical_not(wrapped)))(lambda: update(keys, values))


def merge_kernel(place_ref, direct_ref, passed_ref, out_ref, *, count):
    last = place_ref[0] == count - 1

    @pl.when(last)
    def _():
        out_ref[...] = direct_ref[...]

    @pl.when(jnp.logical_not(last))
    def _():
        out_ref[...] = passed_ref[...]


def step_kernel(place_ref, q_ref, f_ref, *refs, step, turn, count, q_heads, kv_heads):
    b_ref = refs[0] if turn else None
    state = refs[-3:]
    fold(
        place_ref[0], step, turn, count, f_ref, b_ref,
        lambda keys, values: each_head(q_ref, keys, values, *state, q_heads, kv_heads, False),
    )


def last_kernel(place_ref, q_ref, f_ref, residual_ref, gain_ref, *refs, step, q_heads, kv_heads):
    acc_ref, total_ref, top_ref, out_ref, square_ref = refs[-5:]
    rows, width = out_ref.shape
    square_ref[...] = jnp.zeros(square_ref.shape, jnp.float32)

    def finish(head, acc, total):
        attended = (acc / jnp.sum(total, axis=1, keepdims=True)).astype(jnp.bfloat16).astype(jnp.float32)
        at = pl.ds(pl.multiple_of(head * HEAD_WIDTH, HEAD_WIDTH), HEAD_WIDTH)
        hidden = residual_ref[:, at].astype(jnp.float32) + attended
        acc_ref[head] = hidden
        square_ref[...] = square_ref[...] + hidden * hidden

    wide = f_ref.shape[1] // 2
    behind = place_ref[0] >= step

    @pl.when(behind)
    def _():
        each_head(
            q_ref, ((f_ref, 0),), ((f_ref, wide),), acc_ref, total_ref, top_ref, q_heads, kv_heads, False, finish
        )

    @pl.when(jnp.logical_not(behind))
    def _():
        def one_head(head, carry):
            finish(head, acc_ref[head], total_ref[head])
            return carry

        lax.fori_loop(0, q_heads, one_head, 0)

    square = square_ref[...]
    inv_rms = lax.rsqrt(jnp.sum(square, axis=1, keepdims=True) / width + NORM_EPS)
    inv_rms = jnp.broadcast_to(inv_rms, (rows, HEAD_WIDTH))
    for head in range(q_heads):
        at = slice(head * HEAD_WIDTH, (head + 1) * HEAD_WIDTH)
        out_ref[:, at] = (acc_ref[head] * inv_rms * gain_ref[:, at]).astype(jnp.bfloat16)


def plan(count):
    wrapped = count * 6 // 16
    forward = count - 1 - wrapped
    folds = [min(2 * turn, forward - 1 - (wrapped - turn)) for turn in range(1, wrapped + 1)]
    return forward, wrapped, folds


def forward_pairs(count, step):
    return [(i, i + 1) for i in range(step - 1, count - 1)]


def pass_pairs(count, turn):
    return [(count - 1 - i, count - 2 - i) for i in range(turn)]


def shift(array, pairs):
    return lax.ppermute(array, "seq", pairs)


def layer(queries, keys, values, residual, norm_gain):
    count = lax.axis_size("seq")
    forward_steps, wrapped_blocks, folds = plan(count)
    query = queries[0]
    rows, width = query.shape
    q_heads = width // HEAD_WIDTH
    kv_heads = keys.shape[2] // HEAD_WIDTH
    place = lax.axis_index("seq").astype(jnp.int32).reshape(1)
    own = jnp.concatenate([keys[0], values[0]], axis=1)
    state_shape = (q_heads, rows, HEAD_WIDTH)
    state = pltpu.VMEM(state_shape, jnp.float32)
    vmem = pl.BlockSpec(memory_space=pltpu.VMEM)
    smem = pl.BlockSpec(memory_space=pltpu.SMEM)
    params = pltpu.CompilerParams(vmem_limit_bytes=VMEM_LIMIT)

    def cost(keys_seen):
        return pl.CostEstimate(
            flops=4 * q_heads * rows * keys_seen * HEAD_WIDTH,
            transcendentals=q_heads * rows * keys_seen,
            bytes_accessed=4 * rows * width,
        )

    forward = shift(own, forward_pairs(count, 1))
    direct = [shift(own, [(0, count - 1)])]
    query, acc, total, top = pl.pallas_call(
        functools.partial(first_kernel, q_heads=q_heads, kv_heads=kv_heads),
        out_shape=(pltpu.VMEM(query.shape, query.dtype), state, state, state),
        in_specs=[smem, vmem, vmem],
        out_specs=(vmem, vmem, vmem, vmem),
        compiler_params=params,
        cost_estimate=cost(rows),
        name="first",
    )(place, query, own)
    passed = None
    for step in range(1, forward_steps):
        blocks = (forward,)
        forward = shift(forward, forward_pairs(count, step + 1))
        if step < wrapped_blocks:
            direct.append(shift(own, [(step, count - 1)]))
        turn = folds.index(step) + 1 if step in folds else None
        if turn:
            merged = direct[turn - 1]
            if passed is not None:
                merged = pl.pallas_call(
                    functools.partial(merge_kernel, count=count),
                    out_shape=pltpu.VMEM(own.shape, own.dtype),
                    in_specs=[smem, vmem, vmem],
                    out_specs=vmem,
                    compiler_params=params,
                    cost_estimate=pl.CostEstimate(flops=own.size, transcendentals=0, bytes_accessed=4 * own.size),
                )(place, merged, passed)
            if turn < wrapped_blocks:
                passed = shift(merged, pass_pairs(count, turn))
            blocks = blocks + (merged,)
        at = 2 + len(blocks)
        acc, total, top = pl.pallas_call(
            functools.partial(
                step_kernel, step=step, turn=turn, count=count, q_heads=q_heads, kv_heads=kv_heads
            ),
            out_shape=(state, state, state),
            in_specs=[smem] + [vmem] * (at + 2),
            out_specs=(vmem, vmem, vmem),
            input_output_aliases={at: 0, at + 1: 1, at + 2: 2},
            compiler_params=params,
            cost_estimate=cost(len(blocks) * rows),
        )(place, query, *blocks, acc, total, top)
    _, _, _, normed = pl.pallas_call(
        functools.partial(last_kernel, step=forward_steps, q_heads=q_heads, kv_heads=kv_heads),
        out_shape=(state, state, state, jax.ShapeDtypeStruct((rows, width), jnp.bfloat16)),
        in_specs=[smem] + [vmem] * 7,
        out_specs=(vmem, vmem, vmem, vmem),
        scratch_shapes=[pltpu.VMEM((rows, HEAD_WIDTH), jnp.float32)],
        input_output_aliases={5: 0, 6: 1, 7: 2},
        compiler_params=params,
        cost_estimate=cost(rows),
        name="last",
    )(place, query, forward, residual[0], norm_gain.reshape(1, width), acc, total, top)
    return normed[None]


def solution(mesh):
    placed = P(("groups", "vocab", "batch"), "seq", None)
    return jax.shard_map(
        layer,
        mesh=mesh,
        in_specs=(placed, placed, placed, placed, P()),
        out_specs=placed,
        check_vma=False,
    )
```
